32 devices in a mesh: row: 8 (over y, x, core), col: 4 (over z).
Axes of the slice: x: 2, y: 2, z: 4, core: 2. Of those that a mesh axis runs over, the one named last changes fastest.
Arguments:
- tangents: float32 [192, 128, 6144], P('row', None, 'col'), may hold values from -6 to 6
- base_flow: float32 [192, 128, 192], P('row', None, 'col'), may hold values from -0.0625 to 0.0625
- mode_mask: int32 [192, 192], P('row', 'col'), may hold values 0 or 1
- decay_rates: float32 [128], replicated, may hold values from 1 to 100
- to_eigen: float32 [128, 128], replicated, may hold values from -0.5 to 0.5
- from_eigen: float32 [128, 128], replicated, may hold values from -0.5 to 0.5
Outputs:
- vectors: float32 [192, 128, 6144], P('row', None, 'col')
- growth: float32 [32], replicated
The draws below stay inside these ranges and needn't reach their ends.
Inputs may be any that keep to these rules, and one draw needn't show every extreme that they name: `mode_mask`: 1 keeps a mode pair of the linearized product, 0 removes it.
All inputs are finite; a program needn't handle non-finite values. No bound on the sum of `mode_mask` on one device may be relied on, other than what follows from the above.
Results may differ from the reference program's by a relative error of at most 0.00005.
Values sent between devices are 32-bit elements; how exact they have to be, the bound alone decides.
A program may use at most 256 MiB of HBM per device.

```python
import math
import jax
import jax.numpy as jnp
from jax import lax

NX = 192
NY = 128
NZ = 192
NV = 32


def plant(values, rng, least, top_value):
    longest = values.shape.index(max(values.shape))
    spots = []
    for shift in (0, 1):
        where = [jax.random.randint(jax.random.fold_in(rng, axis), (), 0, length) for axis, length in enumerate(values.shape)]
        where[longest] = (where[longest] + shift) % values.shape[longest]
        spots.append(tuple(where))
    return values.at[spots[0]].set(least).at[spots[1]].set(top_value)


def block_scale(rng, shape, pieces, least, high):
    factor_of, own = 1.0, jax.random.fold_in(rng, 6)
    for axis_at, parts in pieces:
        heights = jnp.exp(jax.random.uniform(jax.random.fold_in(own, axis_at), (parts,), jnp.float32, least / len(pieces), high / len(pieces)))
        factor_of = factor_of * jnp.repeat(heights, shape[axis_at] // parts).reshape([-1 if axis == axis_at else 1 for axis in range(len(shape))])
    return factor_of


def centred(rng, dims, deviation, most, cuts=(), kind=jnp.bfloat16):
    drawn = deviation * jax.random.normal(rng, dims, jnp.float32)
    if cuts:
        drawn = drawn * block_scale(rng, dims, cuts, -0.22, 0.18)
    return jnp.clip(drawn, -most, most).astype(kind)


def setup_inputs(seed: int = 0) -> dict:
    key_list = jax.random.split(jax.random.key(seed), 7)
    tangents = centred(key_list[0], (NX, NY, NZ * NV), 1.0, 6.0, ((0, 8), (2, 4)), jnp.float32)
    base_flow = centred(key_list[1], (NX, NY, NZ), (NX * NZ // 4) ** -0.5, 0.0625, ((0, 8), (2, 4)), jnp.float32)
    mode_mask = plant((jax.random.randint(key_list[2], (NX, NZ), 0, 4) < 3).astype(jnp.int32), jax.random.fold_in(key_list[2], 1), 0, 1)
    decay_rates = jnp.clip(jnp.exp(jax.random.uniform(key_list[3], (NY,), jnp.float32, math.log(1.0), math.log(100.0))), 1.0, 100.0)
    to_eigen = centred(key_list[4], (NY, NY), NY ** -0.5, 0.5, (), jnp.float32)
    from_eigen = centred(key_list[5], (NY, NY), NY ** -0.5, 0.5, (), jnp.float32)
    return dict(tangents=tangents, base_flow=base_flow, mode_mask=mode_mask, decay_rates=decay_rates, to_eigen=to_eigen, from_eigen=from_eigen)


PRECISE = lax.Precision.HIGHEST
STEP_COEF = 10.0
VISCOSITY = 0.01
ALPHA_X = 0.5
BETA_Z = 1.0

def local_waves(points_count, first_index, length):
    indices = first_index + jnp.arange(length, dtype=jnp.int32)
    middle = points_count // 2
    return jnp.where(indices <= middle, indices, indices - middle).astype(jnp.float32)

def synthesis(points_count):
    points = jnp.arange(points_count, dtype=jnp.int32)[:, None]
    mode_index = jnp.arange(points_count, dtype=jnp.int32)[None, :]
    middle = points_count // 2
    wave_index = jnp.where(mode_index <= middle, mode_index, mode_index - middle)
    turn_count = (points * wave_index % points_count).astype(jnp.float32)
    angles = turn_count * (2.0 * math.pi / points_count)
    return jnp.where(mode_index <= middle, jnp.cos(angles), jnp.sin(angles))

def analysis(points_count):
    mode_index = jnp.arange(points_count, dtype=jnp.int32)
    middle = points_count // 2
    weights = jnp.where((mode_index == 0) | (mode_index == middle), jnp.float32(1.0 / points_count), jnp.float32(2.0 / points_count))
    return weights[:, None] * synthesis(points_count).T

def derivative_analysis(points_count, wave_scale):
    rows_index = jnp.arange(points_count, dtype=jnp.int32)[:, None]
    cols_index = jnp.arange(points_count, dtype=jnp.int32)[None, :]
    middle = points_count // 2
    rising = (cols_index == rows_index + middle) & (rows_index >= 1) & (rows_index < middle)
    falling = (rows_index == cols_index + middle) & (cols_index >= 1) & (cols_index < middle)
    rows_float = jnp.broadcast_to(rows_index.astype(jnp.float32), (points_count, points_count))
    cols_float = jnp.broadcast_to(cols_index.astype(jnp.float32), (points_count, points_count))
    derivative = jnp.where(rising, rows_float, jnp.float32(0.0)) - jnp.where(falling, cols_float, jnp.float32(0.0))
    return -wave_scale * jnp.dot(derivative, analysis(points_count), precision=PRECISE)

def denominators(decay_rates, x_count, z_count, x_start, z_start, x_length, z_length):
    wave_x = ALPHA_X * local_waves(x_count, x_start, x_length)
    wave_z = BETA_Z * local_waves(z_count, z_start, z_length)
    return STEP_COEF + VISCOSITY * (wave_x[:, None, None] ** 2 + wave_z[None, None, :] ** 2) + decay_rates[None, :, None]

def reference(tangents, base_flow, mode_mask, decay_rates, to_eigen, from_eigen):
    x_count, y_count, z_count = base_flow.shape
    vec_count = tangents.shape[2] // z_count
    fields = jnp.transpose(tangents.reshape(x_count, y_count, z_count, vec_count), (3, 0, 1, 2))
    x_synthesis = synthesis(x_count)
    z_synthesis = synthesis(z_count)
    x_derivative = derivative_analysis(x_count, ALPHA_X)
    z_analysis = analysis(z_count)
    speed_field = jnp.einsum('pm,myn->pyn', x_synthesis, base_flow, precision=PRECISE)
    speed_field = jnp.einsum('pyn,sn->pys', speed_field, z_synthesis, precision=PRECISE)
    divisor = denominators(decay_rates, x_count, z_count, 0, 0, x_count, z_count)
    retained = mode_mask.astype(jnp.float32)[:, None, :]

    def advance(one_field):
        physical = jnp.einsum('pm,myn->pyn', x_synthesis, one_field, precision=PRECISE)
        physical = jnp.einsum('pyn,sn->pys', physical, z_synthesis, precision=PRECISE)
        product = speed_field * physical
        returned = jnp.einsum('mp,pys->mys', x_derivative, product, precision=PRECISE)
        returned = jnp.einsum('mys,ns->myn', returned, z_analysis, precision=PRECISE)
        right_side = STEP_COEF * one_field + retained * returned
        eigen_part = jnp.einsum('ji,min->mjn', to_eigen, right_side, precision=PRECISE) / divisor
        return jnp.einsum('yj,mjn->myn', from_eigen, eigen_part, precision=PRECISE)
    stepped = lax.map(advance, fields)
    cell_count = x_count * y_count * z_count
    gram_matrix = jnp.einsum('vmyn,umyn->vu', stepped, stepped, precision=PRECISE) / cell_count
    lower_factor = jnp.linalg.cholesky(gram_matrix)
    identity = jnp.eye(vec_count, dtype=jnp.float32)
    inverse = jax.scipy.linalg.solve_triangular(lower_factor, identity, lower=True)
    orthonormal = jnp.einsum('uv,vmyn->mynu', inverse, stepped, precision=PRECISE)
    growth = jnp.log(jnp.diagonal(lower_factor))
    return (orthonormal.reshape(x_count, y_count, z_count * vec_count), growth)
```

```python
import functools

import jax
import jax.numpy as jnp
import numpy as np
from jax import lax
from jax.experimental import pallas as pl
from jax.experimental.pallas import tpu as pltpu
from jax.sharding import PartitionSpec as P

STEP_COEF = 10.0
VISCOSITY = 0.01
ALPHA_X = 0.5
BETA_Z = 1.0
LANES = 128
MESH = pl.DeviceIdType.MESH


def synthesis(points_count):
    points = np.arange(points_count)[:, None]
    mode_index = np.arange(points_count)[None, :]
    middle = points_count // 2
    wave_index = np.where(mode_index <= middle, mode_index, mode_index - middle)
    angles = (points * wave_index % points_count) * (2.0 * np.pi / points_count)
    return np.where(mode_index <= middle, np.cos(angles), np.sin(angles))


def analysis(points_count):
    mode_index = np.arange(points_count)
    middle = points_count // 2
    weights = np.where((mode_index == 0) | (mode_index == middle), 1.0, 2.0) / points_count
    return weights[:, None] * synthesis(points_count).T


def derivative_analysis(points_count, wave_scale):
    middle = points_count // 2
    derivative = np.zeros((points_count, points_count))
    inner = np.arange(1, middle)
    derivative[inner, middle + inner] = inner
    derivative[middle + inner, inner] = -inner
    return -wave_scale * (derivative @ analysis(points_count))


def split_parts(value):
    high = value.astype(jnp.bfloat16)
    low = (value - high.astype(jnp.float32)).astype(jnp.bfloat16)
    return high, low


def parts_dot(left, right, dims=(((1,), (0,)), ((), ()))):
    left_high, left_low = left
    right_high, right_low = right
    dot = lambda a, b: lax.dot_general(a, b, dims, preferred_element_type=jnp.float32)
    return dot(left_high, right_high) + (dot(left_high, right_low) + dot(left_low, right_high))


def wave_number(index, count):
    return jnp.where(index <= count // 2, index, index - count // 2).astype(jnp.float32)


def substep_kernel(
    row_devices, col_devices, vec_count, lane_parts, row_block,
    q_ref, base_ref, mask_ref, decay_ref, to_ref, from_ref, sx_ref, sp_ref, sz_ref, st_ref, az_ref, gx_ref,
    stepped_ref, gram_ref,
    fields, terms, spectrum, planes, blocks, speed, rows, keep, zwave, rates, old, high_ref, cross_ref, packed, slots,
    field_sem, field_sent, base_sem, base_sent, term_sem, term_sent, old_sem, out_sem, gram_sem, gram_sent,
    *halves
):
    all_devices = row_devices * col_devices
    x_length, y_count, zv_length = q_ref.shape
    part = zv_length // lane_parts
    plane_count = y_count // all_devices
    z_length = zv_length // vec_count
    x_count, z_count = x_length * row_devices, z_length * col_devices
    groups = x_length // row_block * lane_parts
    tiles = zv_length // LANES
    row, col = lax.axis_index("row"), lax.axis_index("col")
    me = row * col_devices + col

    def others(action):
        def visit(i, carry):
            device = lax.rem(me + i, all_devices)
            action(device, (lax.div(device, col_devices), lax.rem(device, col_devices)))
            return carry

        lax.fori_loop(1, all_devices, visit, 0)

    def send(source, target, sent, arrived, place):
        pltpu.make_async_remote_copy(
            src_ref=source, dst_ref=target, send_sem=sent, recv_sem=arrived, device_id=place, device_id_type=MESH
        ).start()

    def whole_wait(ref, semaphore):
        pltpu.make_async_copy(ref, ref, semaphore).wait()

    barrier = pltpu.get_barrier_semaphore()
    others(lambda device, place: pl.semaphore_signal(barrier, inc=1, device_id=place, device_id_type=MESH))
    pl.semaphore_wait(barrier, all_devices - 1)

    def send_fields(k, carry):
        target = fields.at[k, col, row]
        pltpu.make_async_copy(q_ref.at[:, me * plane_count + k, :], target, field_sem.at[k]).start()
        others(
            lambda device, place: send(
                q_ref.at[:, device * plane_count + k, :], target, field_sent, field_sem.at[k], place
            )
        )
        return carry

    send_fields(0, 0)
    spectrum[...] = base_ref[...].T

    def send_base(k, carry):
        target = planes.at[k, col * row_devices + row]
        pltpu.make_async_copy(spectrum.at[me * plane_count + k], target, base_sem).start()
        others(
            lambda device, place: send(
                spectrum.at[device * plane_count + k], target, base_sent, base_sem, place
            )
        )
        return carry

    lax.fori_loop(0, plane_count, send_base, 0)
    lax.fori_loop(1, plane_count, send_fields, 0)

    def place_of(g):
        block, lane_part = lax.div(g, lane_parts), lax.rem(g, lane_parts)
        lanes = pl.ds(pl.multiple_of(lane_part * part, LANES), part)
        some = pl.ds(pl.multiple_of(block * row_block, row_block), row_block)
        return lane_part, slice(None) if row_block == x_length else some, lanes

    def fetch(g):
        lane_part, some, lanes = place_of(g)
        slot = lax.rem(g, 2)
        return pltpu.make_async_copy(q_ref.at[some, :, lanes], old.at[slot], old_sem.at[slot])

    fetch(0).start()

    spread = (
        lax.broadcasted_iota(jnp.int32, (z_length, zv_length), 1) // vec_count
        == lax.broadcasted_iota(jnp.int32, (z_length, zv_length), 0)
    ).astype(jnp.bfloat16)
    kept = jnp.dot(mask_ref[...].astype(jnp.bfloat16), spread, preferred_element_type=jnp.float32)
    lane = lax.broadcasted_iota(jnp.int32, (1, zv_length), 1)
    waves = (BETA_Z * wave_number(col * z_length + lane // vec_count, z_count)) ** 2
    for p in range(lane_parts):
        keep[p] = kept[:, p * part : (p + 1) * part]
        zwave[p] = waves[:, p * part : (p + 1) * part]
    column = jnp.broadcast_to(decay_ref[...], (LANES, y_count)).T
    for t in range(part // LANES):
        rates[:, t * LANES : (t + 1) * LANES] = column
    if rows.shape[0] > x_count:
        rows[x_count:, :] = jnp.zeros((rows.shape[0] - x_count, LANES), jnp.float32)
    high_ref[...] = jnp.zeros_like(high_ref)
    cross_ref[...] = jnp.zeros_like(cross_ref)
    whole_wait(planes, base_sem)

    def plane(k, carry):
        for c in range(col_devices):
            for m in range(x_length):
                blocks[c, m * row_devices : (m + 1) * row_devices, :] = planes[
                    k, c * row_devices : (c + 1) * row_devices, m * z_length : (m + 1) * z_length
                ]
        partial = sum(
            parts_dot(
                split_parts(blocks[c]), split_parts(st_ref[c * z_length : (c + 1) * z_length, :])
            )
            for c in range(col_devices)
        )
        speed[...] = parts_dot(split_parts(partial), split_parts(sp_ref[...]), (((0,), (0,)), ((), ())))
        whole_wait(fields.at[k], field_sem.at[k])

        def gather(t, carry):
            c, lanes = lax.div(t, tiles), pl.ds(pl.multiple_of(lax.rem(t, tiles) * LANES, LANES), LANES)
            for r in range(row_devices):
                rows[r * x_length : (r + 1) * x_length, :] = fields[k, c, r, :, lanes]
            for h, half in enumerate(halves):
                half[pl.ds(pl.multiple_of(t * LANES, LANES), LANES), :] = rows[h * LANES : (h + 1) * LANES, :].T
            return carry

        lax.fori_loop(0, col_devices * tiles, gather, 0)
        sx = split_parts(sx_ref[...])
        sz = split_parts(sz_ref[...])
        az = split_parts(az_ref[...])
        gx = split_parts(gx_ref[...])

        def transform(pair, carry):
            for u in range(2):
                where = pl.ds(pair * 2 + u, z_count, stride=vec_count)
                field = jnp.concatenate([half[where, :] for half in halves], axis=1)
                field = parts_dot(split_parts(field), sx)
                field = parts_dot(sz, split_parts(field))
                field = field * speed[...]
                field = parts_dot(az, split_parts(field))
                field = parts_dot(split_parts(field), gx)
                for h, half in enumerate(halves):
                    half[where, :] = field[:, h * LANES : (h + 1) * LANES]
            return carry

        lax.fori_loop(0, vec_count // 2, transform, 0)

        def scatter(t, carry):
            c, lanes = lax.div(t, tiles), pl.ds(pl.multiple_of(lax.rem(t, tiles) * LANES, LANES), LANES)
            for h, half in enumerate(halves):
                known = min(x_count - h * LANES, LANES)
                flipped = half[pl.ds(pl.multiple_of(t * LANES, LANES), LANES), :].T
                rows[h * LANES : h * LANES + known, :] = flipped[:known]
            for r in range(row_devices):
                fields[k, c, r, :, lanes] = rows[r * x_length : (r + 1) * x_length, :]
            return carry

        lax.fori_loop(0, col_devices * tiles, scatter, 0)

        def send_terms(g, carry):
            lane_part, some, lanes = place_of(g)
            target = terms.at[lane_part, some, me * plane_count + k, :]
            pltpu.make_async_copy(fields.at[k, col, row, some, lanes], target, term_sem.at[g]).start()
            others(
                lambda device, place: send(
                    fields.at[k, place[1], place[0], some, lanes], target, term_sent, term_sem.at[g], place
                )
            )
            return carry

        lax.fori_loop(0, groups, send_terms, 0)
        return carry

    lax.fori_loop(0, plane_count, plane, 0)
    into, back = split_parts(to_ref[...]), split_parts(from_ref[...])
    batch = 2 if row_block % 2 == 0 else 1
    inner = lambda a, b: lax.dot_general(a, b, (((0,), (0,)), ((), ())), preferred_element_type=jnp.float32)

    def group(g, carry):
        lane_part, some, lanes = place_of(g)
        slot = lax.rem(g, 2)
        region = terms.at[lane_part, some]

        @pl.when(g + 1 < groups)
        def _():
            fetch(g + 1).start()

        fetch(g).wait()
        whole_wait(region, term_sem.at[g])
        first = lax.div(g, lane_parts) * row_block

        def advance(b, carry):
            highs, lows = [], []
            for u in range(batch):
                at = b * batch + u
                m = first + at
                right_side = STEP_COEF * old[slot, at] + terms[lane_part, m] * keep[lane_part, pl.ds(m, 1), :]
                wave_x = ALPHA_X * wave_number(row * x_length + m, x_count)
                wave_row = STEP_COEF + VISCOSITY * (wave_x * wave_x + zwave[lane_part])
                eigen_part = parts_dot(into, split_parts(right_side)) / (wave_row + rates[...])
                stepped = parts_dot(back, split_parts(eigen_part))
                terms[lane_part, m] = stepped
                high, low = split_parts(stepped)
                highs.append(high)
                lows.append(low)
            high, low = jnp.concatenate(highs, axis=0), jnp.concatenate(lows, axis=0)
            high_total, cross_total = high_ref[...], cross_ref[...]
            for t in range(part // LANES):
                tile = slice(t * LANES, (t + 1) * LANES)
                high_total += inner(high[:, tile], high[:, tile])
                cross_total += inner(high[:, tile], low[:, tile])
            high_ref[...] = high_total
            cross_ref[...] = cross_total
            return carry

        lax.fori_loop(0, row_block // batch, advance, 0)
        pltpu.make_async_copy(region, stepped_ref.at[some, :, lanes], out_sem).start()
        return carry

    lax.fori_loop(0, groups, group, 0)

    total = high_ref[...] + cross_ref[...] + cross_ref[...].T
    sides = LANES // vec_count
    lane = lax.broadcasted_iota(jnp.int32, (LANES, LANES), 1) // vec_count
    side = lax.broadcasted_iota(jnp.int32, (LANES, LANES), 0) // vec_count
    total = jnp.where(lane == side, total, 0.0)
    folded = sum(total[s * vec_count : (s + 1) * vec_count, :] for s in range(sides))
    folded = sum((pltpu.roll(folded, s * vec_count, 1) for s in range(1, sides)), folded)
    short = vec_count // sides
    packed[...] = sum(
        jnp.where(lane[:short] == s, folded[s * short : (s + 1) * short, :], 0.0) for s in range(sides)
    )
    slots[me] = packed[...]
    others(lambda device, place: send(packed, slots.at[me], gram_sent, gram_sem, place))
    arrived = slots.at[pl.ds(0, all_devices - 1)]
    whole_wait(arrived, gram_sem)
    gram_ref[...] = lax.fori_loop(
        0, all_devices, lambda i, value: value + slots[i], jnp.zeros(gram_ref.shape, jnp.float32)
    )
    whole_wait(arrived, gram_sent)
    whole_wait(terms, out_sem)
    for semaphore in (field_sent, term_sent):
        whole_wait(fields.at[:, pl.ds(0, col_devices - 1)], semaphore)
        whole_wait(fields.at[:, col_devices - 1, pl.ds(0, row_devices - 1)], semaphore)
    sent = y_count - plane_count
    whole_wait(spectrum.at[pl.ds(0, sent // 8 * 8)], base_sent)
    for _ in range(sent % 8):
        whole_wait(spectrum.at[0], base_sent)


def substep(tangents, base_flow, mode_mask, decay_rates, to_eigen, from_eigen, lane_parts):
    x_length, y_count, zv_length = tangents.shape
    z_length = base_flow.shape[2]
    vec_count = zv_length // z_length
    row_devices, col_devices = lax.axis_size("row"), lax.axis_size("col")
    all_devices = row_devices * col_devices
    x_count, z_count = x_length * row_devices, z_length * col_devices
    plane_count = y_count // all_devices
    part = zv_length // lane_parts
    row_block = 8 if x_length % 8 == 0 else x_length
    groups = x_length // row_block * lane_parts
    padded = -(-x_count // LANES) * LANES
    extra = padded - x_count
    table = lambda values: jnp.asarray(values.astype(np.float32))
    widen = lambda values: table(np.pad(values, ((0, extra), (0, extra))))
    sx = synthesis(x_count).T
    by_place = sx.reshape(row_devices, x_length, x_count).swapaxes(0, 1).reshape(x_count, x_count)
    tables = (
        widen(sx),
        table(np.pad(by_place, ((0, 0), (0, extra)))),
        table(synthesis(z_count)),
        table(synthesis(z_count).T),
        table(analysis(z_count)),
        widen(derivative_analysis(x_count, ALPHA_X).T),
    )
    base = jnp.transpose(base_flow, (0, 2, 1)).reshape(x_length * z_length, y_count)
    length = -(-base.shape[0] // LANES) * LANES
    base = jnp.pad(base, ((0, length - base.shape[0]), (0, 0)))
    here = pl.BlockSpec(memory_space=pltpu.VMEM)
    far = pl.BlockSpec(memory_space=pl.ANY)
    real = lambda *shape: pltpu.VMEM(shape, jnp.float32)
    dma = lambda *shape: pltpu.SemaphoreType.DMA(shape) if shape else pltpu.SemaphoreType.DMA
    short = vec_count * vec_count // LANES
    return pl.pallas_call(
        functools.partial(substep_kernel, row_devices, col_devices, vec_count, lane_parts, row_block),
        out_shape=(
            jax.ShapeDtypeStruct(tangents.shape, jnp.float32),
            jax.ShapeDtypeStruct((short, LANES), jnp.float32),
        ),
        in_specs=[far] + [here] * 11,
        out_specs=(far, here),
        scratch_shapes=[
            real(plane_count, col_devices, row_devices, x_length, zv_length),
            real(lane_parts, x_length, y_count, part),
            real(y_count, length),
            real(plane_count, all_devices, length),
            real(col_devices, x_count, z_length),
            real(z_count, padded),
            real(padded, LANES),
            real(lane_parts, x_length, part),
            real(lane_parts, 1, part),
            real(y_count, part),
            real(2, row_block, y_count, part),
            real(LANES, LANES),
            real(LANES, LANES),
            real(short, LANES),
            real(all_devices, short, LANES),
            dma(plane_count),
            dma(),
            dma(),
            dma(),
            dma(groups),
            dma(),
            dma(2),
            dma(),
            dma(),
            dma(),
        ]
        + [real(z_count * vec_count, LANES)] * (padded // LANES),
        compiler_params=pltpu.CompilerParams(
            collective_id=0, has_side_effects=True, vmem_limit_bytes=63 * 1024 * 1024
        ),
    )(tangents, base, mode_mask, decay_rates[None, :], to_eigen, from_eigen, *tables)


def combine_kernel(x_ref, w_ref, o_ref):
    weights = split_parts(w_ref[...])
    width = w_ref.shape[0]
    for g in range(x_ref.shape[2] // width):
        lanes = slice(g * width, (g + 1) * width)
        o_ref[0, :, lanes] = parts_dot(split_parts(x_ref[0, :, lanes]), weights)


def combine(stepped, weights):
    x_length, y_count, zv_length = stepped.shape
    one = pl.BlockSpec((1, y_count, zv_length), lambda m: (m, 0, 0))
    return pl.pallas_call(
        combine_kernel,
        grid=(x_length,),
        out_shape=jax.ShapeDtypeStruct(stepped.shape, jnp.float32),
        in_specs=[one, pl.BlockSpec(weights.shape, lambda m: (0, 0))],
        out_specs=one,
        compiler_params=pltpu.CompilerParams(vmem_limit_bytes=12 * 1024 * 1024),
    )(stepped, weights)


def body(tangents, base_flow, mode_mask, decay_rates, to_eigen, from_eigen):
    x_length, y_count, zv_length = tangents.shape
    z_length = base_flow.shape[2]
    vec_count = zv_length // z_length
    cells = x_length * lax.axis_size("row") * y_count * z_length * lax.axis_size("col")
    stepped, gram = substep(tangents, base_flow, mode_mask, decay_rates, to_eigen, from_eigen, 2)
    sides = LANES // vec_count
    gram_matrix = gram.reshape(vec_count // sides, sides, vec_count).swapaxes(0, 1)
    gram_matrix = gram_matrix.reshape(vec_count, vec_count) / cells
    lower_factor = jnp.linalg.cholesky(gram_matrix)
    identity = jnp.eye(vec_count, dtype=jnp.float32)
    inverse = jax.scipy.linalg.solve_triangular(lower_factor, identity, lower=True)
    width = 2 * LANES if zv_length % (2 * LANES) == 0 else LANES
    weights = jnp.kron(jnp.eye(width // vec_count, dtype=jnp.float32), inverse.T)
    return combine(stepped, weights), jnp.log(jnp.diagonal(lower_factor))


def solution(mesh):
    placed = (P("row", None, "col"), P("row", None, "col"), P("row", "col"), P(), P(), P())
    return jax.shard_map(
        body, mesh=mesh, in_specs=placed, out_specs=(P("row", None, "col"), P()), check_vma=False
    )
```

```python
import functools

import jax
import jax.numpy as jnp
import numpy as np
from jax import lax
from jax.experimental import pallas as pl
from jax.experimental.pallas import tpu as pltpu
from jax.sharding import PartitionSpec as P

STEP_COEF = 10.0
VISCOSITY = 0.01
ALPHA_X = 0.5
BETA_Z = 1.0
LANES = 128
MESH = pl.DeviceIdType.MESH


def synthesis(points_count):
    points = np.arange(points_count)[:, None]
    mode_index = np.arange(points_count)[None, :]
    middle = points_count // 2
    wave_index = np.where(mode_index <= middle, mode_index, mode_index - middle)
    angles = (points * wave_index % points_count) * (2.0 * np.pi / points_count)
    return np.where(mode_index <= middle, np.cos(angles), np.sin(angles))


def analysis(points_count):
    mode_index = np.arange(points_count)
    middle = points_count // 2
    weights = np.where((mode_index == 0) | (mode_index == middle), 1.0, 2.0) / points_count
    return weights[:, None] * synthesis(points_count).T


def derivative_analysis(points_count, wave_scale):
    middle = points_count // 2
    derivative = np.zeros((points_count, points_count))
    inner = np.arange(1, middle)
    derivative[inner, middle + inner] = inner
    derivative[middle + inner, inner] = -inner
    return -wave_scale * (derivative @ analysis(points_count))


def split_parts(value):
    high = value.astype(jnp.bfloat16)
    low = (value - high.astype(jnp.float32)).astype(jnp.bfloat16)
    return high, low


def parts_dot(left, right, dims=(((1,), (0,)), ((), ()))):
    left_high, left_low = left
    right_high, right_low = right
    dot = lambda a, b: lax.dot_general(a, b, dims, preferred_element_type=jnp.float32)
    return dot(left_high, right_high) + (dot(left_high, right_low) + dot(left_low, right_high))


def stacked(left):
    high, low = split_parts(left)
    top = jnp.concatenate([high, high], axis=1)
    return jnp.concatenate([top, jnp.concatenate([low, jnp.zeros_like(low)], axis=1)], axis=0)


def stacked_dot(left, right):
    both = jnp.dot(left, jnp.concatenate(split_parts(right), axis=0), preferred_element_type=jnp.float32)
    return both[: left.shape[0] // 2] + both[left.shape[0] // 2 :]


def wave_number(index, count):
    return jnp.where(index <= count // 2, index, index - count // 2).astype(jnp.float32)


def substep_kernel(
    row_devices, col_devices, vec_count, lane_parts, row_block,
    q_ref, base_ref, mask_ref, decay_ref, to_ref, from_ref, sx_ref, sp_ref, sz_ref, st_ref, az_ref, gx_ref,
    terms, gram_ref,
    fields, spectrum, planes, blocks, speed, rows, keep, zwave, rates, old, both_ref, packed, slots,
    field_sem, field_sent, base_sem, base_sent, term_sem, term_sent, old_sem, gram_sem, gram_sent,
    *halves
):
    all_devices = row_devices * col_devices
    x_length, y_count, zv_length = q_ref.shape
    part = zv_length // lane_parts
    plane_count = y_count // all_devices
    z_length = zv_length // vec_count
    x_count, z_count = x_length * row_devices, z_length * col_devices
    groups = x_length // row_block * lane_parts
    tiles = zv_length // LANES
    row, col = lax.axis_index("row"), lax.axis_index("col")
    me = row * col_devices + col

    def others(action):
        def visit(i, carry):
            device = lax.rem(me + i, all_devices)
            action(device, (lax.div(device, col_devices), lax.rem(device, col_devices)))
            return carry

        lax.fori_loop(1, all_devices, visit, 0)

    def send(source, target, sent, arrived, place):
        pltpu.make_async_remote_copy(
            src_ref=source, dst_ref=target, send_sem=sent, recv_sem=arrived, device_id=place, device_id_type=MESH
        ).start()

    def whole_wait(ref, semaphore):
        pltpu.make_async_copy(ref, ref, semaphore).wait()

    barrier = pltpu.get_barrier_semaphore()
    others(lambda device, place: pl.semaphore_signal(barrier, inc=1, device_id=place, device_id_type=MESH))
    pl.semaphore_wait(barrier, all_devices - 1)

    def send_fields(k, carry):
        target = fields.at[k, col, row]
        pltpu.make_async_copy(q_ref.at[:, me * plane_count + k, :], target, field_sem.at[k]).start()
        others(
            lambda device, place: send(
                q_ref.at[:, device * plane_count + k, :], target, field_sent, field_sem.at[k], place
            )
        )
        return carry

    send_fields(0, 0)
    spectrum[...] = base_ref[...].T

    def send_base(k, carry):
        target = planes.at[k, col * row_devices + row]
        pltpu.make_async_copy(spectrum.at[me * plane_count + k], target, base_sem).start()
        others(
            lambda device, place: send(
                spectrum.at[device * plane_count + k], target, base_sent, base_sem, place
            )
        )
        return carry

    lax.fori_loop(0, plane_count, send_base, 0)
    lax.fori_loop(1, plane_count, send_fields, 0)

    def place_of(g):
        block, lane_part = lax.div(g, lane_parts), lax.rem(g, lane_parts)
        lanes = pl.ds(pl.multiple_of(lane_part * part, LANES), part)
        some = pl.ds(pl.multiple_of(block * row_block, row_block), row_block)
        return lane_part, slice(None) if row_block == x_length else some, lanes

    def fetch(g):
        lane_part, some, lanes = place_of(g)
        slot = lax.rem(g, 2)
        return pltpu.make_async_copy(q_ref.at[some, :, lanes], old.at[slot], old_sem.at[slot])

    fetch(0).start()

    spread = (
        lax.broadcasted_iota(jnp.int32, (z_length, zv_length), 1) // vec_count
        == lax.broadcasted_iota(jnp.int32, (z_length, zv_length), 0)
    ).astype(jnp.bfloat16)
    kept = jnp.dot(mask_ref[...].astype(jnp.bfloat16), spread, preferred_element_type=jnp.float32)
    lane = lax.broadcasted_iota(jnp.int32, (1, zv_length), 1)
    waves = (BETA_Z * wave_number(col * z_length + lane // vec_count, z_count)) ** 2
    for p in range(lane_parts):
        keep[p] = kept[:, p * part : (p + 1) * part]
        zwave[p] = waves[:, p * part : (p + 1) * part]
    column = jnp.broadcast_to(decay_ref[...], (LANES, y_count)).T
    for t in range(part // LANES):
        rates[:, t * LANES : (t + 1) * LANES] = column
    if rows.shape[0] > x_count:
        rows[x_count:, :] = jnp.zeros((rows.shape[0] - x_count, LANES), jnp.float32)
    both_ref[...] = jnp.zeros_like(both_ref)
    whole_wait(planes, base_sem)

    def plane(k, carry):
        for c in range(col_devices):
            for m in range(x_length):
                blocks[c, m * row_devices : (m + 1) * row_devices, :] = planes[
                    k, c * row_devices : (c + 1) * row_devices, m * z_length : (m + 1) * z_length
                ]
        partial = sum(
            parts_dot(
                split_parts(blocks[c]), split_parts(st_ref[c * z_length : (c + 1) * z_length, :])
            )
            for c in range(col_devices)
        )
        speed[...] = parts_dot(split_parts(partial), split_parts(sp_ref[...]), (((0,), (0,)), ((), ())))
        whole_wait(fields.at[k], field_sem.at[k])

        def gather(t, carry):
            c, lanes = lax.div(t, tiles), pl.ds(pl.multiple_of(lax.rem(t, tiles) * LANES, LANES), LANES)
            for r in range(row_devices):
                rows[r * x_length : (r + 1) * x_length, :] = fields[k, c, r, :, lanes]
            for h, half in enumerate(halves):
                half[pl.ds(pl.multiple_of(t * LANES, LANES), LANES), :] = rows[h * LANES : (h + 1) * LANES, :].T
            return carry

        lax.fori_loop(0, col_devices * tiles, gather, 0)
        sx = split_parts(sx_ref[...])
        sz = split_parts(sz_ref[...])
        az = split_parts(az_ref[...])
        gx = split_parts(gx_ref[...])

        def transform(pair, carry):
            for u in range(2):
                where = pl.ds(pair * 2 + u, z_count, stride=vec_count)
                field = jnp.concatenate([half[where, :] for half in halves], axis=1)
                field = parts_dot(split_parts(field), sx)
                field = parts_dot(sz, split_parts(field))
                field = field * speed[...]
                field = parts_dot(az, split_parts(field))
                field = parts_dot(split_parts(field), gx)
                for h, half in enumerate(halves):
                    half[where, :] = field[:, h * LANES : (h + 1) * LANES]
            return carry

        lax.fori_loop(0, vec_count // 2, transform, 0)

        def scatter(t, carry):
            c, lanes = lax.div(t, tiles), pl.ds(pl.multiple_of(lax.rem(t, tiles) * LANES, LANES), LANES)
            for h, half in enumerate(halves):
                known = min(x_count - h * LANES, LANES)
                flipped = half[pl.ds(pl.multiple_of(t * LANES, LANES), LANES), :].T
                rows[h * LANES : h * LANES + known, :] = flipped[:known]
            for r in range(row_devices):
                fields[k, c, r, :, lanes] = rows[r * x_length : (r + 1) * x_length, :]
            return carry

        lax.fori_loop(0, col_devices * tiles, scatter, 0)

        def send_terms(g, carry):
            lane_part, some, lanes = place_of(g)
            target = terms.at[lane_part, some, me * plane_count + k, :]
            pltpu.make_async_copy(fields.at[k, col, row, some, lanes], target, term_sem.at[g]).start()
            others(
                lambda device, place: send(
                    fields.at[k, place[1], place[0], some, lanes], target, term_sent, term_sem.at[g], place
                )
            )
            return carry

        lax.fori_loop(0, groups, send_terms, 0)
        return carry

    lax.fori_loop(0, plane_count, plane, 0)
    into, back = stacked(to_ref[...]), stacked(from_ref[...])
    batch = 2 if row_block % 2 == 0 else 1
    inner = lambda a, b: lax.dot_general(a, b, (((0,), (0,)), ((), ())), preferred_element_type=jnp.float32)

    def group(g, carry):
        lane_part, some, lanes = place_of(g)
        slot = lax.rem(g, 2)
        region = terms.at[lane_part, some]

        @pl.when(g + 1 < groups)
        def _():
            fetch(g + 1).start()

        fetch(g).wait()
        whole_wait(region, term_sem.at[g])
        first = lax.div(g, lane_parts) * row_block

        def advance(b, carry):
            highs, lows = [], []
            for u in range(batch):
                at = b * batch + u
                m = first + at
                right_side = STEP_COEF * old[slot, at] + terms[lane_part, m] * keep[lane_part, pl.ds(m, 1), :]
                wave_x = ALPHA_X * wave_number(row * x_length + m, x_count)
                wave_row = STEP_COEF + VISCOSITY * (wave_x * wave_x + zwave[lane_part])
                eigen_part = stacked_dot(into, right_side) / (wave_row + rates[...])
                stepped = stacked_dot(back, eigen_part)
                terms[lane_part, m] = stepped
                high, low = split_parts(stepped)
                highs.append(high)
                lows.append(low)
            high, low = jnp.concatenate(highs, axis=0), jnp.concatenate(lows, axis=0)
            total = both_ref[...]
            for t in range(part // LANES):
                tile = slice(t * LANES, (t + 1) * LANES)
                total += inner(high[:, tile], jnp.concatenate([high[:, tile], low[:, tile]], axis=1))
            both_ref[...] = total
            return carry

        lax.fori_loop(0, row_block // batch, advance, 0)
        return carry

    lax.fori_loop(0, groups, group, 0)

    cross = both_ref[:, LANES:]
    total = both_ref[:, :LANES] + cross + cross.T
    sides = LANES // vec_count
    lane = lax.broadcasted_iota(jnp.int32, (LANES, LANES), 1) // vec_count
    side = lax.broadcasted_iota(jnp.int32, (LANES, LANES), 0) // vec_count
    total = jnp.where(lane == side, total, 0.0)
    folded = sum(total[s * vec_count : (s + 1) * vec_count, :] for s in range(sides))
    folded = sum((pltpu.roll(folded, s * vec_count, 1) for s in range(1, sides)), folded)
    short = vec_count // sides
    packed[...] = sum(
        jnp.where(lane[:short] == s, folded[s * short : (s + 1) * short, :], 0.0) for s in range(sides)
    )
    slots[me] = packed[...]
    others(lambda device, place: send(packed, slots.at[me], gram_sent, gram_sem, place))
    arrived = slots.at[pl.ds(0, all_devices - 1)]
    whole_wait(arrived, gram_sem)
    gram_ref[...] = lax.fori_loop(
        0, all_devices, lambda i, value: value + slots[i], jnp.zeros(gram_ref.shape, jnp.float32)
    )
    whole_wait(arrived, gram_sent)
    for semaphore in (field_sent, term_sent):
        whole_wait(fields.at[:, pl.ds(0, col_devices - 1)], semaphore)
        whole_wait(fields.at[:, col_devices - 1, pl.ds(0, row_devices - 1)], semaphore)
    sent = y_count - plane_count
    whole_wait(spectrum.at[pl.ds(0, sent // 8 * 8)], base_sent)
    for _ in range(sent % 8):
        whole_wait(spectrum.at[0], base_sent)


def substep(tangents, base_flow, mode_mask, decay_rates, to_eigen, from_eigen, lane_parts):
    x_length, y_count, zv_length = tangents.shape
    z_length = base_flow.shape[2]
    vec_count = zv_length // z_length
    row_devices, col_devices = lax.axis_size("row"), lax.axis_size("col")
    all_devices = row_devices * col_devices
    x_count, z_count = x_length * row_devices, z_length * col_devices
    plane_count = y_count // all_devices
    part = zv_length // lane_parts
    row_block = 8 if x_length % 8 == 0 else x_length
    groups = x_length // row_block * lane_parts
    padded = -(-x_count // LANES) * LANES
    extra = padded - x_count
    table = lambda values: jnp.asarray(values.astype(np.float32))
    widen = lambda values: table(np.pad(values, ((0, extra), (0, extra))))
    sx = synthesis(x_count).T
    by_place = sx.reshape(row_devices, x_length, x_count).swapaxes(0, 1).reshape(x_count, x_count)
    tables = (
        widen(sx),
        table(np.pad(by_place, ((0, 0), (0, extra)))),
        table(synthesis(z_count)),
        table(synthesis(z_count).T),
        table(analysis(z_count)),
        widen(derivative_analysis(x_count, ALPHA_X).T),
    )
    base = jnp.transpose(base_flow, (0, 2, 1)).reshape(x_length * z_length, y_count)
    length = -(-base.shape[0] // LANES) * LANES
    base = jnp.pad(base, ((0, length - base.shape[0]), (0, 0)))
    here = pl.BlockSpec(memory_space=pltpu.VMEM)
    far = pl.BlockSpec(memory_space=pl.ANY)
    real = lambda *shape: pltpu.VMEM(shape, jnp.float32)
    dma = lambda *shape: pltpu.SemaphoreType.DMA(shape) if shape else pltpu.SemaphoreType.DMA
    short = vec_count * vec_count // LANES
    return pl.pallas_call(
        functools.partial(substep_kernel, row_devices, col_devices, vec_count, lane_parts, row_block),
        out_shape=(
            pltpu.VMEM((lane_parts, x_length, y_count, part), jnp.float32),
            pltpu.VMEM((short, LANES), jnp.float32),
        ),
        in_specs=[pl.BlockSpec(memory_space=pltpu.HBM)] + [here] * 11,
        out_specs=(here, here),
        scratch_shapes=[
            real(plane_count, col_devices, row_devices, x_length, zv_length),
            real(y_count, length),
            real(plane_count, all_devices, length),
            real(col_devices, x_count, z_length),
            real(z_count, padded),
            real(padded, LANES),
            real(lane_parts, x_length, part),
            real(lane_parts, 1, part),
            real(y_count, part),
            real(2, row_block, y_count, part),
            real(LANES, 2 * LANES),
            real(short, LANES),
            real(all_devices, short, LANES),
            dma(plane_count),
            dma(),
            dma(),
            dma(),
            dma(groups),
            dma(),
            dma(2),
            dma(),
            dma(),
        ]
        + [real(z_count * vec_count, LANES)] * (padded // LANES),
        compiler_params=pltpu.CompilerParams(
            collective_id=0, has_side_effects=True, vmem_limit_bytes=42 * 1024 * 1024
        ),
    )(tangents, base, mode_mask, decay_rates[None, :], to_eigen, from_eigen, *tables)


def combine_kernel(vec_count, cells, gram_ref, stepped_ref, out_ref, growth_ref, given, weights, give_sem):
    lane_parts, x_length, y_count, part = stepped_ref.shape
    slots = given.shape[0]
    give = lambda i: pltpu.make_async_copy(given.at[lax.rem(i, slots)], out_ref.at[i], give_sem.at[lax.rem(i, slots)])
    sides = LANES // vec_count
    short = vec_count // sides
    lane = lax.broadcasted_iota(jnp.int32, (vec_count, LANES), 1)
    line = lax.broadcasted_iota(jnp.int32, (vec_count, LANES), 0)
    gram = jnp.concatenate(
        [gram_ref[...] if s == 0 else pltpu.roll(gram_ref[...], LANES - s * vec_count, 1) for s in range(sides)], axis=0
    )
    left = jnp.where(lane < vec_count, gram / cells, 0.0)
    right = jnp.where(lane == line, 1.0, 0.0)
    pivots = jnp.zeros((1, LANES), jnp.float32)
    for j in range(vec_count):
        column = jnp.broadcast_to(left[:, j : j + 1], (vec_count, LANES))
        pivot = column[j : j + 1, :]
        factor = jnp.where(line > j, column / pivot, 0.0)
        pivots = jnp.where(lane[:1] == j, pivot, pivots)
        left = left - factor * left[j : j + 1, :]
        right = right - factor * right[j : j + 1, :]
    roots = jnp.sqrt(pivots)
    growth_ref[...] = jnp.log(roots)[:, :vec_count]
    turned = jnp.concatenate([right] + [jnp.zeros((LANES - vec_count, LANES), jnp.float32)], axis=0).T
    inverse = jnp.where(lane < vec_count, turned[:vec_count, :] / roots, 0.0)
    spread = sum((pltpu.roll(inverse, s * vec_count, 1) for s in range(1, sides)), inverse)
    spread = jnp.concatenate([spread] * sides, axis=0)
    across = lax.broadcasted_iota(jnp.int32, (LANES, LANES), 1) // vec_count
    down = lax.broadcasted_iota(jnp.int32, (LANES, LANES), 0) // vec_count
    high, low = split_parts(jnp.where(across == down, spread, 0.0))
    weights[...] = jnp.concatenate(
        [jnp.concatenate([high, low], axis=1), jnp.concatenate([high, jnp.zeros_like(low)], axis=1)], axis=0
    )

    def mix(i, carry):
        @pl.when(i >= slots)
        def _():
            give(i - slots).wait()

        slot = lax.rem(i, slots)
        for p in range(lane_parts):
            lanes = [slice(t * LANES, (t + 1) * LANES) for t in range(part // LANES)]
            whole = jnp.concatenate([stepped_ref[p, i, :, tile] for tile in lanes], axis=0)
            mixed = jnp.dot(
                jnp.concatenate(split_parts(whole), axis=1), weights[...], preferred_element_type=jnp.float32
            )
            mixed = mixed[:, :LANES] + mixed[:, LANES:]
            for t in range(part // LANES):
                first = p * part + t * LANES
                given[slot, :, first : first + LANES] = mixed[t * y_count : (t + 1) * y_count]
        give(i).start()
        return carry

    lax.fori_loop(0, x_length, mix, 0)
    for i in range(max(x_length - slots, 0), x_length):
        give(i).wait()


def combine(stepped, gram, vec_count, cells):
    lane_parts, x_length, y_count, part = stepped.shape
    here = pl.BlockSpec(memory_space=pltpu.VMEM)
    slots = min(6, x_length)
    return pl.pallas_call(
        functools.partial(combine_kernel, vec_count, float(cells)),
        out_shape=(
            jax.ShapeDtypeStruct((x_length, y_count, lane_parts * part), jnp.float32),
            jax.ShapeDtypeStruct((1, vec_count), jnp.float32),
        ),
        in_specs=[here, here],
        out_specs=(pl.BlockSpec(memory_space=pltpu.HBM), here),
        scratch_shapes=[
            pltpu.VMEM((slots, y_count, lane_parts * part), jnp.float32),
            pltpu.VMEM((2 * LANES, 2 * LANES), jnp.bfloat16),
            pltpu.SemaphoreType.DMA((slots,)),
        ],
        compiler_params=pltpu.CompilerParams(vmem_limit_bytes=16 * 1024 * 1024),
    )(gram, stepped)


def body(tangents, base_flow, mode_mask, decay_rates, to_eigen, from_eigen):
    x_length, y_count, zv_length = tangents.shape
    z_length = base_flow.shape[2]
    vec_count = zv_length // z_length
    cells = x_length * lax.axis_size("row") * y_count * z_length * lax.axis_size("col")
    lane_parts = max(p for p in range(1, 5) if zv_length // LANES % p == 0)
    stepped, gram = substep(tangents, base_flow, mode_mask, decay_rates, to_eigen, from_eigen, lane_parts)
    vectors, growth = combine(stepped, gram, vec_count, cells)
    return vectors, growth[0]


def solution(mesh):
    placed = (P("row", None, "col"), P("row", None, "col"), P("row", "col"), P(), P(), P())
    return jax.shard_map(
        body, mesh=mesh, in_specs=placed, out_specs=(P("row", None, "col"), P()), check_vma=False
    )
```

```python
import functools

import jax
import jax.numpy as jnp
import numpy as np
from jax import lax
from jax.experimental import pallas as pl
from jax.experimental.pallas import tpu as pltpu
from jax.sharding import PartitionSpec as P

STEP_COEF = 10.0
VISCOSITY = 0.01
ALPHA_X = 0.5
BETA_Z = 1.0
LANES = 128
MESH = pl.DeviceIdType.MESH


def synthesis(points_count):
    points = np.arange(points_count)[:, None]
    mode_index = np.arange(points_count)[None, :]
    middle = points_count // 2
    wave_index = np.where(mode_index <= middle, mode_index, mode_index - middle)
    angles = (points * wave_index % points_count) * (2.0 * np.pi / points_count)
    return np.where(mode_index <= middle, np.cos(angles), np.sin(angles))


def analysis(points_count):
    mode_index = np.arange(points_count)
    middle = points_count // 2
    weights = np.where((mode_index == 0) | (mode_index == middle), 1.0, 2.0) / points_count
    return weights[:, None] * synthesis(points_count).T


def derivative_analysis(points_count, wave_scale):
    middle = points_count // 2
    derivative = np.zeros((points_count, points_count))
    inner = np.arange(1, middle)
    derivative[inner, middle + inner] = inner
    derivative[middle + inner, inner] = -inner
    return -wave_scale * (derivative @ analysis(points_count))


def split_parts(value):
    high = value.astype(jnp.bfloat16)
    low = (value - high.astype(jnp.float32)).astype(jnp.bfloat16)
    return high, low


def parts_dot(left, right, dims=(((1,), (0,)), ((), ()))):
    left_high, left_low = left
    right_high, right_low = right
    dot = lambda a, b: lax.dot_general(a, b, dims, preferred_element_type=jnp.float32)
    return dot(left_high, right_high) + (dot(left_high, right_low) + dot(left_low, right_high))


def stacked(left):
    high, low = split_parts(left)
    top = jnp.concatenate([high, high], axis=1)
    return jnp.concatenate([top, jnp.concatenate([low, jnp.zeros_like(low)], axis=1)], axis=0)


def stacked_dot(left, right):
    both = jnp.dot(left, jnp.concatenate(split_parts(right), axis=0), preferred_element_type=jnp.float32)
    return both[: left.shape[0] // 2] + both[left.shape[0] // 2 :]


def wave_number(index, count):
    return jnp.where(index <= count // 2, index, index - count // 2).astype(jnp.float32)


def substep_kernel(
    row_devices, col_devices, vec_count, lane_parts, row_block,
    q_ref, base_far, to_far, from_far, sx_far, sp_far, sz_far, st_far, az_far, gx_far, mask_ref, decay_ref,
    terms, gram_ref,
    base_ref, to_ref, from_ref, sx_ref, sp_ref, sz_ref, st_ref, az_ref, gx_ref, fields, spectrum, planes, blocks, speed, rows, keep, zwave, rates, old, both_ref, packed, slots,
    field_sem, field_sent, base_sem, base_sent, term_sem, term_sent, old_sem, gram_sem, gram_sent, load_sem,
    *halves
):
    all_devices = row_devices * col_devices
    x_length, y_count, zv_length = q_ref.shape
    part = zv_length // lane_parts
    plane_count = y_count // all_devices
    z_length = zv_length // vec_count
    x_count, z_count = x_length * row_devices, z_length * col_devices
    groups = x_length // row_block * lane_parts
    tiles = zv_length // LANES
    row, col = lax.axis_index("row"), lax.axis_index("col")
    me = row * col_devices + col

    def others(action):
        def visit(i, carry):
            device = lax.rem(me + i, all_devices)
            action(device, (lax.div(device, col_devices), lax.rem(device, col_devices)))
            return carry

        lax.fori_loop(1, all_devices, visit, 0)

    def send(source, target, sent, arrived, place):
        pltpu.make_async_remote_copy(
            src_ref=source, dst_ref=target, send_sem=sent, recv_sem=arrived, device_id=place, device_id_type=MESH
        ).start()

    def whole_wait(ref, semaphore):
        pltpu.make_async_copy(ref, ref, semaphore).wait()

    loads = [
        pltpu.make_async_copy(source, target, load_sem.at[i])
        for i, (source, target) in enumerate(
            (
                (base_far, base_ref),
                (to_far, to_ref),
                (from_far, from_ref),
                (sx_far, sx_ref),
                (sp_far, sp_ref),
                (sz_far, sz_ref),
                (st_far, st_ref),
                (az_far, az_ref),
                (gx_far, gx_ref),
            )
        )
    ]
    for load in loads:
        load.start()
    barrier = pltpu.get_barrier_semaphore()
    others(lambda device, place: pl.semaphore_signal(barrier, inc=1, device_id=place, device_id_type=MESH))
    pl.semaphore_wait(barrier, all_devices - 1)

    def send_fields(k, carry):
        target = fields.at[k, col, row]
        pltpu.make_async_copy(q_ref.at[:, me * plane_count + k, :], target, field_sem.at[k]).start()
        others(
            lambda device, place: send(
                q_ref.at[:, device * plane_count + k, :], target, field_sent, field_sem.at[k], place
            )
        )
        return carry

    send_fields(0, 0)
    for load in loads:
        load.wait()
    spectrum[...] = base_ref[...].T

    def send_base(k, carry):
        target = planes.at[k, col * row_devices + row]
        pltpu.make_async_copy(spectrum.at[me * plane_count + k], target, base_sem).start()
        others(
            lambda device, place: send(
                spectrum.at[device * plane_count + k], target, base_sent, base_sem, place
            )
        )
        return carry

    lax.fori_loop(0, plane_count, send_base, 0)
    lax.fori_loop(1, plane_count, send_fields, 0)

    def place_of(g):
        block, lane_part = lax.div(g, lane_parts), lax.rem(g, lane_parts)
        lanes = pl.ds(pl.multiple_of(lane_part * part, LANES), part)
        some = pl.ds(pl.multiple_of(block * row_block, row_block), row_block)
        return lane_part, slice(None) if row_block == x_length else some, lanes

    def fetch(g):
        lane_part, some, lanes = place_of(g)
        slot = lax.rem(g, 2)
        return pltpu.make_async_copy(q_ref.at[some, :, lanes], old.at[slot], old_sem.at[slot])

    fetch(0).start()

    spread = (
        lax.broadcasted_iota(jnp.int32, (z_length, zv_length), 1) // vec_count
        == lax.broadcasted_iota(jnp.int32, (z_length, zv_length), 0)
    ).astype(jnp.bfloat16)
    kept = jnp.dot(mask_ref[...].astype(jnp.bfloat16), spread, preferred_element_type=jnp.float32)
    lane = lax.broadcasted_iota(jnp.int32, (1, zv_length), 1)
    waves = (BETA_Z * wave_number(col * z_length + lane // vec_count, z_count)) ** 2
    for p in range(lane_parts):
        keep[p] = kept[:, p * part : (p + 1) * part]
        zwave[p] = waves[:, p * part : (p + 1) * part]
    column = jnp.broadcast_to(decay_ref[...], (LANES, y_count)).T
    for t in range(part // LANES):
        rates[:, t * LANES : (t + 1) * LANES] = column
    if rows.shape[0] > x_count:
        rows[x_count:, :] = jnp.zeros((rows.shape[0] - x_count, LANES), jnp.float32)
    both_ref[...] = jnp.zeros_like(both_ref)
    whole_wait(planes, base_sem)

    def plane(k, carry):
        for c in range(col_devices):
            for m in range(x_length):
                blocks[c, m * row_devices : (m + 1) * row_devices, :] = planes[
                    k, c * row_devices : (c + 1) * row_devices, m * z_length : (m + 1) * z_length
                ]
        partial = sum(
            parts_dot(
                split_parts(blocks[c]), split_parts(st_ref[c * z_length : (c + 1) * z_length, :])
            )
            for c in range(col_devices)
        )
        speed[...] = parts_dot(split_parts(partial), split_parts(sp_ref[...]), (((0,), (0,)), ((), ())))
        whole_wait(fields.at[k], field_sem.at[k])

        def gather(t, carry):
            c, lanes = lax.div(t, tiles), pl.ds(pl.multiple_of(lax.rem(t, tiles) * LANES, LANES), LANES)
            for r in range(row_devices):
                rows[r * x_length : (r + 1) * x_length, :] = fields[k, c, r, :, lanes]
            for h, half in enumerate(halves):
                half[pl.ds(pl.multiple_of(t * LANES, LANES), LANES), :] = rows[h * LANES : (h + 1) * LANES, :].T
            return carry

        lax.fori_loop(0, col_devices * tiles, gather, 0)
        sx = split_parts(sx_ref[...])
        sz = split_parts(sz_ref[...])
        az = split_parts(az_ref[...])
        gx = split_parts(gx_ref[...])

        def transform(pair, carry):
            for u in range(2):
                where = pl.ds(pair * 2 + u, z_count, stride=vec_count)
                field = jnp.concatenate([half[where, :] for half in halves], axis=1)
                field = parts_dot(split_parts(field), sx)
                field = parts_dot(sz, split_parts(field))
                field = field * speed[...]
                field = parts_dot(az, split_parts(field))
                field = parts_dot(split_parts(field), gx)
                for h, half in enumerate(halves):
                    half[where, :] = field[:, h * LANES : (h + 1) * LANES]
            return carry

        lax.fori_loop(0, vec_count // 2, transform, 0)

        def scatter(t, carry):
            c, lanes = lax.div(t, tiles), pl.ds(pl.multiple_of(lax.rem(t, tiles) * LANES, LANES), LANES)
            for h, half in enumerate(halves):
                known = min(x_count - h * LANES, LANES)
                flipped = half[pl.ds(pl.multiple_of(t * LANES, LANES), LANES), :].T
                rows[h * LANES : h * LANES + known, :] = flipped[:known]
            for r in range(row_devices):
                fields[k, c, r, :, lanes] = rows[r * x_length : (r + 1) * x_length, :]
            return carry

        lax.fori_loop(0, col_devices * tiles, scatter, 0)

        def send_terms(g, carry):
            lane_part, some, lanes = place_of(g)
            target = terms.at[lane_part, some, me * plane_count + k, :]
            pltpu.make_async_copy(fields.at[k, col, row, some, lanes], target, term_sem.at[g]).start()
            others(
                lambda device, place: send(
                    fields.at[k, place[1], place[0], some, lanes], target, term_sent, term_sem.at[g], place
                )
            )
            return carry

        lax.fori_loop(0, groups, send_terms, 0)
        return carry

    lax.fori_loop(0, plane_count, plane, 0)
    into, back = stacked(to_ref[...]), stacked(from_ref[...])
    batch = 2 if row_block % 2 == 0 else 1
    inner = lambda a, b: lax.dot_general(a, b, (((0,), (0,)), ((), ())), preferred_element_type=jnp.float32)

    def group(g, carry):
        lane_part, some, lanes = place_of(g)
        slot = lax.rem(g, 2)
        region = terms.at[lane_part, some]

        @pl.when(g + 1 < groups)
        def _():
            fetch(g + 1).start()

        fetch(g).wait()
        whole_wait(region, term_sem.at[g])
        first = lax.div(g, lane_parts) * row_block

        def advance(b, carry):
            highs, lows = [], []
            for u in range(batch):
                at = b * batch + u
                m = first + at
                right_side = STEP_COEF * old[slot, at] + terms[lane_part, m] * keep[lane_part, pl.ds(m, 1), :]
                wave_x = ALPHA_X * wave_number(row * x_length + m, x_count)
                wave_row = STEP_COEF + VISCOSITY * (wave_x * wave_x + zwave[lane_part])
                eigen_part = stacked_dot(into, right_side) / (wave_row + rates[...])
                stepped = stacked_dot(back, eigen_part)
                terms[lane_part, m] = stepped
                high, low = split_parts(stepped)
                highs.append(high)
                lows.append(low)
            high, low = jnp.concatenate(highs, axis=0), jnp.concatenate(lows, axis=0)
            total = both_ref[...]
            for t in range(part // LANES):
                tile = slice(t * LANES, (t + 1) * LANES)
                total += inner(high[:, tile], jnp.concatenate([high[:, tile], low[:, tile]], axis=1))
            both_ref[...] = total
            return carry

        lax.fori_loop(0, row_block // batch, advance, 0)
        return carry

    lax.fori_loop(0, groups, group, 0)

    cross = both_ref[:, LANES:]
    total = both_ref[:, :LANES] + cross + cross.T
    sides = LANES // vec_count
    lane = lax.broadcasted_iota(jnp.int32, (LANES, LANES), 1) // vec_count
    side = lax.broadcasted_iota(jnp.int32, (LANES, LANES), 0) // vec_count
    total = jnp.where(lane == side, total, 0.0)
    folded = sum(total[s * vec_count : (s + 1) * vec_count, :] for s in range(sides))
    folded = sum((pltpu.roll(folded, s * vec_count, 1) for s in range(1, sides)), folded)
    short = vec_count // sides
    packed[...] = sum(
        jnp.where(lane[:short] == s, folded[s * short : (s + 1) * short, :], 0.0) for s in range(sides)
    )
    slots[me] = packed[...]
    others(lambda device, place: send(packed, slots.at[me], gram_sent, gram_sem, place))
    arrived = slots.at[pl.ds(0, all_devices - 1)]
    whole_wait(arrived, gram_sem)
    gram_ref[...] = lax.fori_loop(
        0, all_devices, lambda i, value: value + slots[i], jnp.zeros(gram_ref.shape, jnp.float32)
    )
    whole_wait(arrived, gram_sent)
    for semaphore in (field_sent, term_sent):
        whole_wait(fields.at[:, pl.ds(0, col_devices - 1)], semaphore)
        whole_wait(fields.at[:, col_devices - 1, pl.ds(0, row_devices - 1)], semaphore)
    sent = y_count - plane_count
    whole_wait(spectrum.at[pl.ds(0, sent // 8 * 8)], base_sent)
    for _ in range(sent % 8):
        whole_wait(spectrum.at[0], base_sent)


def substep(tangents, base_flow, mode_mask, decay_rates, to_eigen, from_eigen, lane_parts):
    x_length, y_count, zv_length = tangents.shape
    z_length = base_flow.shape[2]
    vec_count = zv_length // z_length
    row_devices, col_devices = lax.axis_size("row"), lax.axis_size("col")
    all_devices = row_devices * col_devices
    x_count, z_count = x_length * row_devices, z_length * col_devices
    plane_count = y_count // all_devices
    part = zv_length // lane_parts
    row_block = 8 if x_length % 8 == 0 else x_length
    groups = x_length // row_block * lane_parts
    padded = -(-x_count // LANES) * LANES
    extra = padded - x_count
    table = lambda values: jnp.asarray(values.astype(np.float32))
    widen = lambda values: table(np.pad(values, ((0, extra), (0, extra))))
    sx = synthesis(x_count).T
    by_place = sx.reshape(row_devices, x_length, x_count).swapaxes(0, 1).reshape(x_count, x_count)
    tables = (
        widen(sx),
        table(np.pad(by_place, ((0, 0), (0, extra)))),
        table(synthesis(z_count)),
        table(synthesis(z_count).T),
        table(analysis(z_count)),
        widen(derivative_analysis(x_count, ALPHA_X).T),
    )
    base = jnp.transpose(base_flow, (0, 2, 1)).reshape(x_length * z_length, y_count)
    length = -(-base.shape[0] // LANES) * LANES
    base = jnp.pad(base, ((0, length - base.shape[0]), (0, 0)))
    here = pl.BlockSpec(memory_space=pltpu.VMEM)
    far = pl.BlockSpec(memory_space=pltpu.HBM)
    loaded = (base, to_eigen, from_eigen) + tables
    real = lambda *shape: pltpu.VMEM(shape, jnp.float32)
    dma = lambda *shape: pltpu.SemaphoreType.DMA(shape) if shape else pltpu.SemaphoreType.DMA
    short = vec_count * vec_count // LANES
    return pl.pallas_call(
        functools.partial(substep_kernel, row_devices, col_devices, vec_count, lane_parts, row_block),
        out_shape=(
            pltpu.VMEM((lane_parts, x_length, y_count, part), jnp.float32),
            pltpu.VMEM((short, LANES), jnp.float32),
        ),
        in_specs=[far] * (1 + len(loaded)) + [here] * 2,
        out_specs=(here, here),
        scratch_shapes=[real(*value.shape) for value in loaded]
        + [
            real(plane_count, col_devices, row_devices, x_length, zv_length),
            real(y_count, length),
            real(plane_count, all_devices, length),
            real(col_devices, x_count, z_length),
            real(z_count, padded),
            real(padded, LANES),
            real(lane_parts, x_length, part),
            real(lane_parts, 1, part),
            real(y_count, part),
            real(2, row_block, y_count, part),
            real(LANES, 2 * LANES),
            real(short, LANES),
            real(all_devices, short, LANES),
            dma(plane_count),
            dma(),
            dma(),
            dma(),
            dma(groups),
            dma(),
            dma(2),
            dma(),
            dma(),
            dma(len(loaded)),
        ]
        + [real(z_count * vec_count, LANES)] * (padded // LANES),
        compiler_params=pltpu.CompilerParams(
            collective_id=0, has_side_effects=True, vmem_limit_bytes=42 * 1024 * 1024
        ),
    )(tangents, *loaded, mode_mask, decay_rates[None, :])


def combine_kernel(vec_count, cells, gram_ref, stepped_ref, out_ref, growth_ref, given, weights, give_sem):
    lane_parts, x_length, y_count, part = stepped_ref.shape
    slots, depth = given.shape[:2]
    some = lambda i: pl.ds(i * depth, depth)
    give = lambda i: pltpu.make_async_copy(given.at[lax.rem(i, slots)], out_ref.at[some(i)], give_sem.at[lax.rem(i, slots)])
    sides = LANES // vec_count
    short = vec_count // sides
    lane = lax.broadcasted_iota(jnp.int32, (vec_count, LANES), 1)
    line = lax.broadcasted_iota(jnp.int32, (vec_count, LANES), 0)
    gram = jnp.concatenate(
        [gram_ref[...] if s == 0 else pltpu.roll(gram_ref[...], LANES - s * vec_count, 1) for s in range(sides)], axis=0
    )
    left = jnp.where(lane < vec_count, gram / cells, 0.0)
    right = jnp.where(lane == line, 1.0, 0.0)
    pivots = jnp.zeros((1, LANES), jnp.float32)
    block = 8
    for first in range(0, vec_count, block):
        columns = [jnp.broadcast_to(left[:, first + a : first + a + 1], (vec_count, LANES)) for a in range(block)]
        for a in range(block):
            j = first + a
            pivot = columns[a][j : j + 1, :]
            factor = jnp.where(line > j, columns[a] * (1.0 / pivot), 0.0)
            pivots = jnp.where(lane[:1] == j, pivot, pivots)
            for b in range(a + 1, block):
                columns[b] = columns[b] - factor * columns[b][j : j + 1, :]
            left = left - factor * left[j : j + 1, :]
            right = right - factor * right[j : j + 1, :]
    roots = jnp.sqrt(pivots)
    growth_ref[...] = jnp.log(roots)[:, :vec_count]
    turned = jnp.concatenate([right] + [jnp.zeros((LANES - vec_count, LANES), jnp.float32)], axis=0).T
    inverse = jnp.where(lane < vec_count, turned[:vec_count, :] / roots, 0.0)
    spread = sum((pltpu.roll(inverse, s * vec_count, 1) for s in range(1, sides)), inverse)
    spread = jnp.concatenate([spread] * sides, axis=0)
    across = lax.broadcasted_iota(jnp.int32, (LANES, LANES), 1) // vec_count
    down = lax.broadcasted_iota(jnp.int32, (LANES, LANES), 0) // vec_count
    high, low = split_parts(jnp.where(across == down, spread, 0.0))
    weights[...] = jnp.concatenate(
        [jnp.concatenate([high, low], axis=1), jnp.concatenate([high, jnp.zeros_like(low)], axis=1)], axis=0
    )

    def mix(i, carry):
        @pl.when(i >= slots)
        def _():
            give(i - slots).wait()

        slot = lax.rem(i, slots)
        tiles = [(p, slice(t * LANES, (t + 1) * LANES)) for p in range(lane_parts) for t in range(part // LANES)]
        for b in range(depth):
            m = i * depth + b
            whole = jnp.concatenate([stepped_ref[p, m, :, tile] for p, tile in tiles], axis=0)
            mixed = jnp.dot(
                jnp.concatenate(split_parts(whole), axis=1), weights[...], preferred_element_type=jnp.float32
            )
            mixed = mixed[:, :LANES] + mixed[:, LANES:]
            for t in range(len(tiles)):
                given[slot, b, :, t * LANES : (t + 1) * LANES] = mixed[t * y_count : (t + 1) * y_count]
        give(i).start()
        return carry

    blocks = x_length // depth
    lax.fori_loop(0, blocks, mix, 0)
    for i in range(max(blocks - slots, 0), blocks):
        give(i).wait()


def combine(stepped, gram, vec_count, cells):
    lane_parts, x_length, y_count, part = stepped.shape
    here = pl.BlockSpec(memory_space=pltpu.VMEM)
    depth = 4 if x_length % 4 == 0 else 1
    slots = min(4, x_length // depth)
    return pl.pallas_call(
        functools.partial(combine_kernel, vec_count, float(cells)),
        out_shape=(
            jax.ShapeDtypeStruct((x_length, y_count, lane_parts * part), jnp.float32),
            jax.ShapeDtypeStruct((1, vec_count), jnp.float32),
        ),
        in_specs=[here, here],
        out_specs=(pl.BlockSpec(memory_space=pltpu.HBM), here),
        scratch_shapes=[
            pltpu.VMEM((slots, depth, y_count, lane_parts * part), jnp.float32),
            pltpu.VMEM((2 * LANES, 2 * LANES), jnp.bfloat16),
            pltpu.SemaphoreType.DMA((slots,)),
        ],
        compiler_params=pltpu.CompilerParams(vmem_limit_bytes=16 * 1024 * 1024),
    )(gram, stepped)


def body(tangents, base_flow, mode_mask, decay_rates, to_eigen, from_eigen):
    x_length, y_count, zv_length = tangents.shape
    z_length = base_flow.shape[2]
    vec_count = zv_length // z_length
    cells = x_length * lax.axis_size("row") * y_count * z_length * lax.axis_size("col")
    lane_parts = max(p for p in range(1, 5) if zv_length // LANES % p == 0)
    stepped, gram = substep(tangents, base_flow, mode_mask, decay_rates, to_eigen, from_eigen, lane_parts)
    vectors, growth = combine(stepped, gram, vec_count, cells)
    return vectors, growth[0]


def solution(mesh):
    placed = (P("row", None, "col"), P("row", None, "col"), P("row", "col"), P(), P(), P())
    return jax.shard_map(
        body, mesh=mesh, in_specs=placed, out_specs=(P("row", None, "col"), P()), check_vma=False
    )
```

```python
import functools

import jax
import jax.numpy as jnp
import numpy as np
from jax import lax
from jax.experimental import pallas as pl
from jax.experimental.pallas import tpu as pltpu
from jax.sharding import PartitionSpec as P

STEP_COEF = 10.0
VISCOSITY = 0.01
ALPHA_X = 0.5
BETA_Z = 1.0
LANES = 128
MESH = pl.DeviceIdType.MESH


def synthesis(points_count):
    points = np.arange(points_count)[:, None]
    mode_index = np.arange(points_count)[None, :]
    middle = points_count // 2
    wave_index = np.where(mode_index <= middle, mode_index, mode_index - middle)
    angles = (points * wave_index % points_count) * (2.0 * np.pi / points_count)
    return np.where(mode_index <= middle, np.cos(angles), np.sin(angles))


def analysis(points_count):
    mode_index = np.arange(points_count)
    middle = points_count // 2
    weights = np.where((mode_index == 0) | (mode_index == middle), 1.0, 2.0) / points_count
    return weights[:, None] * synthesis(points_count).T


def derivative_analysis(points_count, wave_scale):
    middle = points_count // 2
    derivative = np.zeros((points_count, points_count))
    inner = np.arange(1, middle)
    derivative[inner, middle + inner] = inner
    derivative[middle + inner, inner] = -inner
    return -wave_scale * (derivative @ analysis(points_count))


def split_parts(value):
    high = value.astype(jnp.bfloat16)
    low = (value - high.astype(jnp.float32)).astype(jnp.bfloat16)
    return high, low


def parts_dot(left, right, dims=(((1,), (0,)), ((), ()))):
    left_high, left_low = left
    right_high, right_low = right
    dot = lambda a, b: lax.dot_general(a, b, dims, preferred_element_type=jnp.float32)
    return dot(left_high, right_high) + (dot(left_high, right_low) + dot(left_low, right_high))


def stacked(left):
    high, low = split_parts(left)
    top = jnp.concatenate([high, high], axis=1)
    return jnp.concatenate([top, jnp.concatenate([low, jnp.zeros_like(low)], axis=1)], axis=0)


def stacked_dot(left, right):
    both = jnp.dot(left, jnp.concatenate(split_parts(right), axis=0), preferred_element_type=jnp.float32)
    return both[: left.shape[0] // 2] + both[left.shape[0] // 2 :]


def wave_number(index, count):
    return jnp.where(index <= count // 2, index, index - count // 2).astype(jnp.float32)


def substep_kernel(
    row_devices, col_devices, vec_count, lane_parts, row_block,
    q_ref, base_far, to_far, from_far, sx_far, sp_far, sz_far, st_far, az_far, gx_far, mask_ref, decay_ref,
    terms, gram_ref,
    base_ref, to_ref, from_ref, sx_ref, sp_ref, sz_ref, st_ref, az_ref, gx_ref, fields, spectrum, planes, blocks, speed, rows, keep, zwave, rates, old, both_ref, packed, slots,
    field_sem, field_sent, base_sem, base_sent, term_sem, term_sent, old_sem, gram_sem, gram_sent, load_sem,
    *halves
):
    all_devices = row_devices * col_devices
    x_length, y_count, zv_length = q_ref.shape
    part = zv_length // lane_parts
    plane_count = y_count // all_devices
    z_length = zv_length // vec_count
    x_count, z_count = x_length * row_devices, z_length * col_devices
    groups = x_length // row_block * lane_parts
    tiles = zv_length // LANES
    row, col = lax.axis_index("row"), lax.axis_index("col")
    me = row * col_devices + col

    def others(action):
        def visit(i, carry):
            device = lax.rem(me + i, all_devices)
            action(device, (lax.div(device, col_devices), lax.rem(device, col_devices)))
            return carry

        lax.fori_loop(1, all_devices, visit, 0)

    def send(source, target, sent, arrived, place):
        pltpu.make_async_remote_copy(
            src_ref=source, dst_ref=target, send_sem=sent, recv_sem=arrived, device_id=place, device_id_type=MESH
        ).start()

    def whole_wait(ref, semaphore):
        pltpu.make_async_copy(ref, ref, semaphore).wait()

    loads = [
        pltpu.make_async_copy(source, target, load_sem.at[i])
        for i, (source, target) in enumerate(
            (
                (base_far, base_ref),
                (to_far, to_ref),
                (from_far, from_ref),
                (sx_far, sx_ref),
                (sp_far, sp_ref),
                (sz_far, sz_ref),
                (st_far, st_ref),
                (az_far, az_ref),
                (gx_far, gx_ref),
            )
        )
    ]
    for load in loads:
        load.start()
    barrier = pltpu.get_barrier_semaphore()
    others(lambda device, place: pl.semaphore_signal(barrier, inc=1, device_id=place, device_id_type=MESH))
    pl.semaphore_wait(barrier, all_devices - 1)

    def send_fields(k, carry):
        target = fields.at[k, col, row]
        pltpu.make_async_copy(q_ref.at[:, me * plane_count + k, :], target, field_sem.at[k]).start()
        others(
            lambda device, place: send(
                q_ref.at[:, device * plane_count + k, :], target, field_sent, field_sem.at[k], place
            )
        )
        return carry

    send_fields(0, 0)
    for load in loads:
        load.wait()
    spectrum[...] = base_ref[...].T

    def send_base(k, carry):
        target = planes.at[k, col * row_devices + row]
        pltpu.make_async_copy(spectrum.at[me * plane_count + k], target, base_sem).start()
        others(
            lambda device, place: send(
                spectrum.at[device * plane_count + k], target, base_sent, base_sem, place
            )
        )
        return carry

    lax.fori_loop(0, plane_count, send_base, 0)
    lax.fori_loop(1, plane_count, send_fields, 0)

    def place_of(g):
        block, lane_part = lax.div(g, lane_parts), lax.rem(g, lane_parts)
        lanes = pl.ds(pl.multiple_of(lane_part * part, LANES), part)
        some = pl.ds(pl.multiple_of(block * row_block, row_block), row_block)
        return lane_part, slice(None) if row_block == x_length else some, lanes

    def fetch(g):
        lane_part, some, lanes = place_of(g)
        slot = lax.rem(g, 2)
        return pltpu.make_async_copy(q_ref.at[some, :, lanes], old.at[slot], old_sem.at[slot])

    fetch(0).start()

    spread = (
        lax.broadcasted_iota(jnp.int32, (z_length, zv_length), 1) // vec_count
        == lax.broadcasted_iota(jnp.int32, (z_length, zv_length), 0)
    ).astype(jnp.bfloat16)
    kept = jnp.dot(mask_ref[...].astype(jnp.bfloat16), spread, preferred_element_type=jnp.float32)
    lane = lax.broadcasted_iota(jnp.int32, (1, zv_length), 1)
    waves = (BETA_Z * wave_number(col * z_length + lane // vec_count, z_count)) ** 2
    for p in range(lane_parts):
        keep[p] = kept[:, p * part : (p + 1) * part]
        zwave[p] = waves[:, p * part : (p + 1) * part]
    column = jnp.broadcast_to(decay_ref[...], (LANES, y_count)).T
    for t in range(part // LANES):
        rates[:, t * LANES : (t + 1) * LANES] = column
    if rows.shape[0] > x_count:
        rows[x_count:, :] = jnp.zeros((rows.shape[0] - x_count, LANES), jnp.float32)
    both_ref[...] = jnp.zeros_like(both_ref)
    whole_wait(planes, base_sem)

    def plane(k, carry):
        for c in range(col_devices):
            for m in range(x_length):
                blocks[c, m * row_devices : (m + 1) * row_devices, :] = planes[
                    k, c * row_devices : (c + 1) * row_devices, m * z_length : (m + 1) * z_length
                ]
        partial = sum(
            parts_dot(
                split_parts(blocks[c]), split_parts(st_ref[c * z_length : (c + 1) * z_length, :])
            )
            for c in range(col_devices)
        )
        speed[...] = parts_dot(split_parts(partial), split_parts(sp_ref[...]), (((0,), (0,)), ((), ())))
        whole_wait(fields.at[k], field_sem.at[k])

        def gather(t, carry):
            c, lanes = lax.div(t, tiles), pl.ds(pl.multiple_of(lax.rem(t, tiles) * LANES, LANES), LANES)
            for r in range(row_devices):
                rows[r * x_length : (r + 1) * x_length, :] = fields[k, c, r, :, lanes]
            for h, half in enumerate(halves):
                half[pl.ds(pl.multiple_of(t * LANES, LANES), LANES), :] = rows[h * LANES : (h + 1) * LANES, :].T
            return carry

        lax.fori_loop(0, col_devices * tiles, gather, 0)
        sx = split_parts(sx_ref[...])
        sz = split_parts(sz_ref[...])
        az = split_parts(az_ref[...])
        gx = split_parts(gx_ref[...])

        def transform(pair, carry):
            for u in range(2):
                where = pl.ds(pair * 2 + u, z_count, stride=vec_count)
                field = jnp.concatenate([half[where, :] for half in halves], axis=1)
                field = parts_dot(split_parts(field), sx)
                field = parts_dot(sz, split_parts(field))
                field = field * speed[...]
                field = parts_dot(az, split_parts(field))
                field = parts_dot(split_parts(field), gx)
                for h, half in enumerate(halves):
                    half[where, :] = field[:, h * LANES : (h + 1) * LANES]
            return carry

        lax.fori_loop(0, vec_count // 2, transform, 0)

        def scatter(t, carry):
            c, lanes = lax.div(t, tiles), pl.ds(pl.multiple_of(lax.rem(t, tiles) * LANES, LANES), LANES)
            for h, half in enumerate(halves):
                known = min(x_count - h * LANES, LANES)
                flipped = half[pl.ds(pl.multiple_of(t * LANES, LANES), LANES), :].T
                rows[h * LANES : h * LANES + known, :] = flipped[:known]
            for r in range(row_devices):
                fields[k, c, r, :, lanes] = rows[r * x_length : (r + 1) * x_length, :]
            return carry

        lax.fori_loop(0, col_devices * tiles, scatter, 0)

        def send_terms(g, carry):
            lane_part, some, lanes = place_of(g)
            target = terms.at[lane_part, some, me * plane_count + k, :]
            pltpu.make_async_copy(fields.at[k, col, row, some, lanes], target, term_sem.at[g]).start()
            others(
                lambda device, place: send(
                    fields.at[k, place[1], place[0], some, lanes], target, term_sent, term_sem.at[g], place
                )
            )
            return carry

        lax.fori_loop(0, groups, send_terms, 0)
        return carry

    lax.fori_loop(0, plane_count, plane, 0)
    into, back = stacked(to_ref[...]), stacked(from_ref[...])
    batch = 4 if row_block % 4 == 0 else 1
    inner = lambda a, b: lax.dot_general(a, b, (((0,), (0,)), ((), ())), preferred_element_type=jnp.float32)

    def group(g, carry):
        lane_part, some, lanes = place_of(g)
        slot = lax.rem(g, 2)
        region = terms.at[lane_part, some]

        @pl.when(g + 1 < groups)
        def _():
            fetch(g + 1).start()

        fetch(g).wait()
        whole_wait(region, term_sem.at[g])
        first = lax.div(g, lane_parts) * row_block

        def advance(b, carry):
            highs, lows = [], []
            for u in range(batch):
                at = b * batch + u
                m = first + at
                right_side = STEP_COEF * old[slot, at] + terms[lane_part, m] * keep[lane_part, pl.ds(m, 1), :]
                wave_x = ALPHA_X * wave_number(row * x_length + m, x_count)
                wave_row = STEP_COEF + VISCOSITY * (wave_x * wave_x + zwave[lane_part])
                eigen_part = stacked_dot(into, right_side) / (wave_row + rates[...])
                stepped = stacked_dot(back, eigen_part)
                terms[lane_part, m] = stepped
                high, low = split_parts(stepped)
                highs.append(high)
                lows.append(low)
            high, low = jnp.concatenate(highs, axis=0), jnp.concatenate(lows, axis=0)
            total = both_ref[...]
            for t in range(part // LANES):
                tile = slice(t * LANES, (t + 1) * LANES)
                total += inner(high[:, tile], jnp.concatenate([high[:, tile], low[:, tile]], axis=1))
            both_ref[...] = total
            return carry

        lax.fori_loop(0, row_block // batch, advance, 0)
        return carry

    lax.fori_loop(0, groups, group, 0)

    cross = both_ref[:, LANES:]
    total = both_ref[:, :LANES] + cross + cross.T
    sides = LANES // vec_count
    lane = lax.broadcasted_iota(jnp.int32, (LANES, LANES), 1) // vec_count
    side = lax.broadcasted_iota(jnp.int32, (LANES, LANES), 0) // vec_count
    total = jnp.where(lane == side, total, 0.0)
    folded = sum(total[s * vec_count : (s + 1) * vec_count, :] for s in range(sides))
    folded = sum((pltpu.roll(folded, s * vec_count, 1) for s in range(1, sides)), folded)
    short = vec_count // sides
    packed[...] = sum(
        jnp.where(lane[:short] == s, folded[s * short : (s + 1) * short, :], 0.0) for s in range(sides)
    )
    slots[me] = packed[...]
    others(lambda device, place: send(packed, slots.at[me], gram_sent, gram_sem, place))
    arrived = slots.at[pl.ds(0, all_devices - 1)]
    whole_wait(arrived, gram_sem)
    gram_ref[...] = lax.fori_loop(
        0, all_devices, lambda i, value: value + slots[i], jnp.zeros(gram_ref.shape, jnp.float32)
    )
    whole_wait(arrived, gram_sent)
    for semaphore in (field_sent, term_sent):
        whole_wait(fields.at[:, pl.ds(0, col_devices - 1)], semaphore)
        whole_wait(fields.at[:, col_devices - 1, pl.ds(0, row_devices - 1)], semaphore)
    sent = y_count - plane_count
    whole_wait(spectrum.at[pl.ds(0, sent // 8 * 8)], base_sent)
    for _ in range(sent % 8):
        whole_wait(spectrum.at[0], base_sent)


def substep(tangents, base_flow, mode_mask, decay_rates, to_eigen, from_eigen, lane_parts):
    x_length, y_count, zv_length = tangents.shape
    z_length = base_flow.shape[2]
    vec_count = zv_length // z_length
    row_devices, col_devices = lax.axis_size("row"), lax.axis_size("col")
    all_devices = row_devices * col_devices
    x_count, z_count = x_length * row_devices, z_length * col_devices
    plane_count = y_count // all_devices
    part = zv_length // lane_parts
    row_block = 8 if x_length % 8 == 0 else x_length
    groups = x_length // row_block * lane_parts
    padded = -(-x_count // LANES) * LANES
    extra = padded - x_count
    table = lambda values: jnp.asarray(values.astype(np.float32))
    widen = lambda values: table(np.pad(values, ((0, extra), (0, extra))))
    sx = synthesis(x_count).T
    by_place = sx.reshape(row_devices, x_length, x_count).swapaxes(0, 1).reshape(x_count, x_count)
    tables = (
        widen(sx),
        table(np.pad(by_place, ((0, 0), (0, extra)))),
        table(synthesis(z_count)),
        table(synthesis(z_count).T),
        table(analysis(z_count)),
        widen(derivative_analysis(x_count, ALPHA_X).T),
    )
    base = jnp.transpose(base_flow, (0, 2, 1)).reshape(x_length * z_length, y_count)
    length = -(-base.shape[0] // LANES) * LANES
    base = jnp.pad(base, ((0, length - base.shape[0]), (0, 0)))
    here = pl.BlockSpec(memory_space=pltpu.VMEM)
    far = pl.BlockSpec(memory_space=pltpu.HBM)
    loaded = (base, to_eigen, from_eigen) + tables
    real = lambda *shape: pltpu.VMEM(shape, jnp.float32)
    dma = lambda *shape: pltpu.SemaphoreType.DMA(shape) if shape else pltpu.SemaphoreType.DMA
    short = vec_count * vec_count // LANES
    return pl.pallas_call(
        functools.partial(substep_kernel, row_devices, col_devices, vec_count, lane_parts, row_block),
        out_shape=(
            pltpu.VMEM((lane_parts, x_length, y_count, part), jnp.float32),
            pltpu.VMEM((short, LANES), jnp.float32),
        ),
        in_specs=[far] * (1 + len(loaded)) + [here] * 2,
        out_specs=(here, here),
        scratch_shapes=[real(*value.shape) for value in loaded]
        + [
            real(plane_count, col_devices, row_devices, x_length, zv_length),
            real(y_count, length),
            real(plane_count, all_devices, length),
            real(col_devices, x_count, z_length),
            real(z_count, padded),
            real(padded, LANES),
            real(lane_parts, x_length, part),
            real(lane_parts, 1, part),
            real(y_count, part),
            real(2, row_block, y_count, part),
            real(LANES, 2 * LANES),
            real(short, LANES),
            real(all_devices, short, LANES),
            dma(plane_count),
            dma(),
            dma(),
            dma(),
            dma(groups),
            dma(),
            dma(2),
            dma(),
            dma(),
            dma(len(loaded)),
        ]
        + [real(z_count * vec_count, LANES)] * (padded // LANES),
        compiler_params=pltpu.CompilerParams(
            collective_id=0, has_side_effects=True, vmem_limit_bytes=42 * 1024 * 1024
        ),
    )(tangents, *loaded, mode_mask, decay_rates[None, :])


def combine_kernel(vec_count, cells, gram_ref, stepped_ref, out_ref, growth_ref, given, weights, give_sem):
    lane_parts, x_length, y_count, part = stepped_ref.shape
    slots, depth = given.shape[:2]
    some = lambda i: pl.ds(i * depth, depth)
    give = lambda i: pltpu.make_async_copy(given.at[lax.rem(i, slots)], out_ref.at[some(i)], give_sem.at[lax.rem(i, slots)])
    sides = LANES // vec_count
    short = vec_count // sides
    lane = lax.broadcasted_iota(jnp.int32, (vec_count, LANES), 1)
    line = lax.broadcasted_iota(jnp.int32, (vec_count, LANES), 0)
    gram = jnp.concatenate(
        [gram_ref[...] if s == 0 else pltpu.roll(gram_ref[...], LANES - s * vec_count, 1) for s in range(sides)], axis=0
    )
    left = jnp.where(lane < vec_count, gram / cells, 0.0)
    right = jnp.where(lane == line, 1.0, 0.0)
    pivots = jnp.zeros((1, LANES), jnp.float32)
    block = 8
    for first in range(0, vec_count, block):
        columns = [jnp.broadcast_to(left[:, first + a : first + a + 1], (vec_count, LANES)) for a in range(block)]
        for a in range(block):
            j = first + a
            pivot = columns[a][j : j + 1, :]
            factor = jnp.where(line > j, columns[a] * (1.0 / pivot), 0.0)
            pivots = jnp.where(lane[:1] == j, pivot, pivots)
            for b in range(a + 1, block):
                columns[b] = columns[b] - factor * columns[b][j : j + 1, :]
            left = left - factor * left[j : j + 1, :]
            right = right - factor * right[j : j + 1, :]
    roots = jnp.sqrt(pivots)
    growth_ref[...] = jnp.log(roots)[:, :vec_count]
    turned = jnp.concatenate([right] + [jnp.zeros((LANES - vec_count, LANES), jnp.float32)], axis=0).T
    inverse = jnp.where(lane < vec_count, turned[:vec_count, :] / roots, 0.0)
    spread = sum((pltpu.roll(inverse, s * vec_count, 1) for s in range(1, sides)), inverse)
    spread = jnp.concatenate([spread] * sides, axis=0)
    across = lax.broadcasted_iota(jnp.int32, (LANES, LANES), 1) // vec_count
    down = lax.broadcasted_iota(jnp.int32, (LANES, LANES), 0) // vec_count
    high, low = split_parts(jnp.where(across == down, spread, 0.0))
    weights[...] = jnp.concatenate(
        [jnp.concatenate([high, low], axis=1), jnp.concatenate([high, jnp.zeros_like(low)], axis=1)], axis=0
    )

    def mix(i, carry):
        @pl.when(i >= slots)
        def _():
            give(i - slots).wait()

        slot = lax.rem(i, slots)
        tiles = [(p, slice(t * LANES, (t + 1) * LANES)) for p in range(lane_parts) for t in range(part // LANES)]
        for b in range(depth):
            m = i * depth + b
            whole = jnp.concatenate([stepped_ref[p, m, :, tile] for p, tile in tiles], axis=0)
            mixed = jnp.dot(
                jnp.concatenate(split_parts(whole), axis=1), weights[...], preferred_element_type=jnp.float32
            )
            mixed = mixed[:, :LANES] + mixed[:, LANES:]
            for t in range(len(tiles)):
                given[slot, b, :, t * LANES : (t + 1) * LANES] = mixed[t * y_count : (t + 1) * y_count]
        give(i).start()
        return carry

    blocks = x_length // depth
    lax.fori_loop(0, blocks, mix, 0)
    for i in range(max(blocks - slots, 0), blocks):
        give(i).wait()


def combine(stepped, gram, vec_count, cells):
    lane_parts, x_length, y_count, part = stepped.shape
    here = pl.BlockSpec(memory_space=pltpu.VMEM)
    depth = 4 if x_length % 4 == 0 else 1
    slots = min(4, x_length // depth)
    return pl.pallas_call(
        functools.partial(combine_kernel, vec_count, float(cells)),
        out_shape=(
            jax.ShapeDtypeStruct((x_length, y_count, lane_parts * part), jnp.float32),
            jax.ShapeDtypeStruct((1, vec_count), jnp.float32),
        ),
        in_specs=[here, here],
        out_specs=(pl.BlockSpec(memory_space=pltpu.HBM), here),
        scratch_shapes=[
            pltpu.VMEM((slots, depth, y_count, lane_parts * part), jnp.float32),
            pltpu.VMEM((2 * LANES, 2 * LANES), jnp.bfloat16),
            pltpu.SemaphoreType.DMA((slots,)),
        ],
        compiler_params=pltpu.CompilerParams(vmem_limit_bytes=16 * 1024 * 1024),
    )(gram, stepped)


def body(tangents, base_flow, mode_mask, decay_rates, to_eigen, from_eigen):
    x_length, y_count, zv_length = tangents.shape
    z_length = base_flow.shape[2]
    vec_count = zv_length // z_length
    cells = x_length * lax.axis_size("row") * y_count * z_length * lax.axis_size("col")
    lane_parts = max(p for p in range(1, 7) if zv_length // LANES % p == 0)
    stepped, gram = substep(tangents, base_flow, mode_mask, decay_rates, to_eigen, from_eigen, lane_parts)
    vectors, growth = combine(stepped, gram, vec_count, cells)
    return vectors, growth[0]


def solution(mesh):
    placed = (P("row", None, "col"), P("row", None, "col"), P("row", "col"), P(), P(), P())
    return jax.shard_map(
        body, mesh=mesh, in_specs=placed, out_specs=(P("row", None, "col"), P()), check_vma=False
    )
```
